32 devices in a mesh: clusters: 2 (over x), blk: 16 (over z, y, core).
Axes of the slice: x: 2, y: 2, z: 4, core: 2. Of those that a mesh axis runs over, the one named last changes fastest.
Arguments:
- positions: float32 [3, 65536], P(None, ('clusters', 'blk')), parts along dimension 1, may hold values from -6 to 6
- velocities: float32 [3, 65536], P(None, ('clusters', 'blk')), parts along dimension 1, may hold values from -6 to 6
- masses: float32 [65536], P(('clusters', 'blk')), parts along dimension 0, may hold values from 0.000390625 to 0.00390625
- active: int32 [8192], P(('clusters', 'blk')), parts along dimension 0, may hold values from 0 to 32767, as said below
Outputs:
- new_positions: float32 [3, 8192], P(None, ('clusters', 'blk')), parts along dimension 1
- new_velocities: float32 [3, 8192], P(None, ('clusters', 'blk')), parts along dimension 1
- accelerations: float32 [3, 8192], P(None, ('clusters', 'blk')), parts along dimension 1
- jerks: float32 [3, 8192], P(None, ('clusters', 'blk')), parts along dimension 1
The draws below stay inside these ranges and needn't reach their ends.
There are 2 independent parts, one for each index of `clusters`. The reference program is written for one: setup_inputs(seed, part) draws one part's arguments, and reference() takes and returns one part's arrays. A program takes and returns all parts, laid end to end along the dimension named above; each array names one. Nothing has to cross between parts.
Inputs may be any that keep to these rules, and one draw needn't show every extreme that they name: Entries b * 256 to (b + 1) * 256 - 1 of active name distinct stars among b * 2048 to (b + 1) * 2048 - 1, for every block b.
All inputs are finite; a program needn't handle non-finite values.
Results may differ from the reference program's by a relative error of at most 0.00023.
Values sent between devices are 32-bit elements; how exact they have to be, the bound alone decides.
A program may use at most 64 MiB of HBM per device.

```python
import math
import jax
import jax.numpy as jnp
from jax import lax

ACT_DEV = 256
STARS_DEV = 2048
ACTIVE = 4096
STARS = 32768
STEPS = 2


def draw_active(key, part):
    blocks = ACTIVE // ACT_DEV

    def one_block(index):
        block_key = jax.random.fold_in(key, index)
        inner = jax.random.permutation(block_key, STARS_DEV - 2)[:ACT_DEV - 2].astype(jnp.int32) + 1
        chosen = jnp.concatenate([inner, jnp.array([0, STARS_DEV - 1], jnp.int32)])
        order = jax.random.permutation(jax.random.fold_in(block_key, 7), ACT_DEV)
        return chosen[order] + index * STARS_DEV
    return jax.vmap(one_block)(jnp.arange(blocks, dtype=jnp.int32)).reshape(-1).astype(jnp.int32)


def levels(key, dims, shards, low, high):
    level = 1.0
    for position, shards_of in shards:
        draws = jax.random.uniform(jax.random.fold_in(jax.random.fold_in(key, 6), position), (shards_of,), jnp.float32, low / len(shards), high / len(shards))
        level = level * jnp.repeat(jnp.exp(draws), dims[position] // shards_of).reshape((-1,) + (1,) * (len(dims) - 1 - position))
    return level


def noise(rng, extent, scale, limit, split=(), kind=jnp.bfloat16):
    values = scale * jax.random.normal(rng, extent, jnp.float32)
    if split:
        values = values * levels(rng, extent, split, -0.22, 0.18)
    return jnp.clip(values, -limit, limit).astype(kind)


def setup_inputs(seed: int = 0, part: int = 0) -> dict:
    keys = jax.random.split(jax.random.key(seed), 5)
    part_splits = jax.random.split(jax.random.fold_in(keys[4], part), 5)
    positions = noise(part_splits[0], (3, STARS), 1.0, 6.0, ((1, 16),), jnp.float32)
    velocities = noise(part_splits[1], (3, STARS), 1.0, 6.0, ((1, 16),), jnp.float32)
    masses = jnp.clip(jnp.exp(math.log(0.00390625) - 2.3025851 * jax.random.uniform(part_splits[2], (STARS,), jnp.float32) ** levels(part_splits[2], (STARS,), ((0, 16),), -0.2, 0.2)), 0.000390625, 0.00390625)
    active = draw_active(jax.random.fold_in(jax.random.fold_in(keys[4], part), 71), part)
    return dict(positions=positions, velocities=velocities, masses=masses, active=active)


def pair_terms(target_pos, target_vel, source):
    separation = source[0:3, None, :] - target_pos[:, :, None]
    closing = source[3:6, None, :] - target_vel[:, :, None]
    squared = lax.optimization_barrier(jnp.sum(separation * separation, axis=0)) + 0.0025
    inverse = lax.rsqrt(squared)
    weight = source[6][None, :] * inverse * inverse * inverse
    radial = lax.optimization_barrier(jnp.sum(separation * closing, axis=0))
    accel = lax.optimization_barrier(jnp.sum(weight[None] * separation, axis=-1))
    jerk = lax.optimization_barrier(jnp.sum(weight[None] * (closing - 3.0 * (radial / squared)[None] * separation), axis=-1))
    return (accel, jerk)

def field(pos, vel, mass):
    source = jnp.concatenate([pos, vel, mass[None, :]], axis=0)
    blocks = ACTIVE // ACT_DEV
    stacked = jnp.concatenate([pos, vel], axis=0).reshape(6, blocks, ACT_DEV).transpose(1, 0, 2)

    def one_block(target):
        return pair_terms(target[0:3], target[3:6], source)
    accel, jerk = lax.map(one_block, stacked)
    accel = accel.transpose(1, 0, 2).reshape(3, ACTIVE)
    jerk = jerk.transpose(1, 0, 2).reshape(3, ACTIVE)
    return (accel, jerk)

def reference(positions, velocities, masses, active):
    time_step = 0.03125
    pos = jnp.take(positions, active, axis=1)
    vel = jnp.take(velocities, active, axis=1)
    mass = jnp.take(masses, active, axis=0)
    accel, jerk = field(pos, vel, mass)
    for section in range(STEPS):
        pred_pos = pos + time_step * vel + time_step ** 2 / 2.0 * accel + time_step ** 3 / 6.0 * jerk
        pred_vel = vel + time_step * accel + time_step ** 2 / 2.0 * jerk
        accel_new, jerk_new = field(pred_pos, pred_vel, mass)
        vel_new = vel + time_step / 2.0 * (accel + accel_new) + time_step ** 2 / 12.0 * (jerk - jerk_new)
        pos_new = pos + time_step / 2.0 * (vel + vel_new) + time_step ** 2 / 12.0 * (accel - accel_new)
        pos, vel, accel, jerk = (pos_new, vel_new, accel_new, jerk_new)
    return (pos, vel, accel, jerk)
```

```python
import functools

import jax
import jax.numpy as jnp
from jax import lax
from jax.experimental import pallas as pl
from jax.experimental.pallas import tpu as pltpu
from jax.sharding import PartitionSpec as P

STEPS = 2
TIME_STEP = 0.03125
ROWS = 32
F32 = jnp.float32
BF16 = jnp.bfloat16


def split3(value):
    high = value.astype(BF16)
    rest = value - high.astype(F32)
    middle = rest.astype(BF16)
    low = (rest - middle.astype(F32)).astype(BF16)
    return [high, middle, low]


def kernel(
    n,
    pos_ref,
    vel_ref,
    mass_ref,
    idx_ref,
    pos_out,
    vel_out,
    accel_out,
    jerk_out,
    slots,
    target,
    even,
    odd,
    right_even,
    right_odd,
    total,
    send_sem,
    recv_sem,
):
    me = lax.axis_index("blk")
    act = idx_ref.shape[1]
    stars = pos_ref.shape[1]

    def peer_of(j):
        offset = ((j + 1) // 2) * (2 * (j % 2) - 1)
        return (me + offset + n) % n

    barrier = pltpu.get_barrier_semaphore()

    @pl.loop(1, n)
    def _(j):
        pl.semaphore_signal(
            barrier,
            inc=1,
            device_id={"blk": peer_of(j)},
            device_id_type=pl.DeviceIdType.MESH,
        )

    local_idx = idx_ref[...] - me * stars
    table = jnp.concatenate(
        [pos_ref[...], vel_ref[...], mass_ref[...], jnp.zeros((1, stars), F32)], axis=0
    )
    pieces = jnp.concatenate(split3(table), axis=0)
    picked = (lax.broadcasted_iota(jnp.int32, (stars, act), 0) == local_idx).astype(F32).astype(BF16)
    found = jnp.dot(pieces, picked, preferred_element_type=F32)
    own = found[0:8] + found[8:16] + found[16:24]
    mass_rows = own[6:8]

    pl.semaphore_wait(barrier, n - 1)

    def copy_to(step, j):
        return pltpu.make_async_remote_copy(
            src_ref=slots.at[step, me],
            dst_ref=slots.at[step, me],
            send_sem=send_sem.at[step, j],
            recv_sem=recv_sem.at[step, me],
            device_id={"blk": peer_of(j)},
            device_id_type=pl.DeviceIdType.MESH,
        )

    def wait_from(step, j):
        peer = peer_of(j)
        pltpu.make_async_remote_copy(
            src_ref=slots.at[step, peer],
            dst_ref=slots.at[step, peer],
            send_sem=send_sem.at[step, j],
            recv_sem=recv_sem.at[step, peer],
            device_id={"blk": peer},
            device_id_type=pl.DeviceIdType.MESH,
        ).wait_recv()

    row_id = lax.broadcasted_iota(jnp.int32, (8, act), 0)

    def weigh(source, weights, right, centre):
        for half in range(act // 128):
            lanes = slice(half * 128, half * 128 + 128)
            src = [source[c : c + 1, lanes] for c in range(6)]
            for top in range(0, act, ROWS):
                rows = slice(top, top + ROWS)
                d = [src[c] - target[c, rows, :] for c in range(3)]
                e = [src[c + 3] - target[c + 3, rows, :] for c in range(3)]
                squared = d[0] * d[0] + d[1] * d[1] + d[2] * d[2] + 0.0025
                radial = d[0] * e[0] + d[1] * e[1] + d[2] * e[2]
                inverse = lax.rsqrt(squared)
                inverse2 = inverse * inverse
                w = inverse2 * inverse
                b = w * inverse2 * radial
                for value, down in ((w, 0), (b, act)):
                    high = value.astype(BF16)
                    low = (value - high.astype(F32)).astype(BF16)
                    out = slice(down + top, down + top + ROWS)
                    weights[out, lanes] = high
                    weights[out, act + half * 128 : act + half * 128 + 128] = low
        factor = jnp.where(row_id == 6, 1.0, source - centre)
        splits = jnp.concatenate(split3(factor * source[6:7]), axis=0)
        right[...] = jnp.concatenate([splits, splits], axis=1)

    def gather_sums(weights, right):
        total[...] += lax.dot_general(
            weights[...],
            right[...],
            (((1,), (1,)), ((), ())),
            preferred_element_type=F32,
        )

    def field(step, own):
        slots[step, me] = own

        @pl.loop(1, n)
        def _(k):
            copy_to(step, n - k).start()

        columns = own.T
        for c in range(6):
            target[c] = jnp.broadcast_to(columns[:, c : c + 1], (act, 128))
        centre = jnp.where(row_id[:, 0:1] < 6, jnp.mean(own, axis=1, keepdims=True), 0.0)
        total[...] = jnp.zeros_like(total)
        odd[...] = jnp.zeros_like(odd)
        right_odd[...] = jnp.zeros_like(right_odd)

        @pl.loop(0, n // 2)
        def _(pair):
            first = 2 * pair

            @pl.when(pair > 0)
            def _():
                wait_from(step, first)

            wait_from(step, first + 1)
            gather_sums(odd, right_odd)
            weigh(slots[step, peer_of(first)], even, right_even, centre)
            gather_sums(even, right_even)
            weigh(slots[step, peer_of(first + 1)], odd, right_odd, centre)

        gather_sums(odd, right_odd)
        sums = total[...].T
        sums = sums[0:8] + sums[8:16] + sums[16:24]
        plain, scaled = sums[:, 0:act], sums[:, act:]
        about = own - centre
        accel = plain[0:3] - about[0:3] * plain[6:7]
        jerk = (
            plain[3:6]
            - about[3:6] * plain[6:7]
            - 3.0 * (scaled[0:3] - about[0:3] * scaled[6:7])
        )
        return accel, jerk

    pos, vel = own[0:3], own[3:6]
    accel, jerk = field(0, own)
    h = TIME_STEP
    for step in range(STEPS):
        pred_pos = pos + h * vel + h**2 / 2.0 * accel + h**3 / 6.0 * jerk
        pred_vel = vel + h * accel + h**2 / 2.0 * jerk
        accel_new, jerk_new = field(
            step + 1, jnp.concatenate([pred_pos, pred_vel, mass_rows], axis=0)
        )
        vel_new = vel + h / 2.0 * (accel + accel_new) + h**2 / 12.0 * (jerk - jerk_new)
        pos = pos + h / 2.0 * (vel + vel_new) + h**2 / 12.0 * (accel - accel_new)
        vel, accel, jerk = vel_new, accel_new, jerk_new
    pos_out[...] = pos
    vel_out[...] = vel
    accel_out[...] = accel
    jerk_out[...] = jerk

    for step in range(STEPS + 1):

        @pl.loop(1, n)
        def _(j):
            copy_to(step, j).wait_send()


def solution(mesh):
    n = mesh.shape["blk"]

    def shards(positions, velocities, masses, active):
        act = active.shape[0]
        vmem = pl.BlockSpec(memory_space=pltpu.VMEM)
        return pl.pallas_call(
            functools.partial(kernel, n),
            out_shape=[jax.ShapeDtypeStruct((3, act), F32)] * 4,
            in_specs=[vmem] * 4,
            out_specs=[vmem] * 4,
            scratch_shapes=[
                pltpu.VMEM((STEPS + 1, n, 8, act), F32),
                pltpu.VMEM((6, act, 128), F32),
                pltpu.VMEM((2 * act, 2 * act), BF16),
                pltpu.VMEM((2 * act, 2 * act), BF16),
                pltpu.VMEM((24, 2 * act), BF16),
                pltpu.VMEM((24, 2 * act), BF16),
                pltpu.VMEM((2 * act, 24), F32),
                pltpu.SemaphoreType.DMA((STEPS + 1, n)),
                pltpu.SemaphoreType.DMA((STEPS + 1, n)),
            ],
            compiler_params=pltpu.CompilerParams(collective_id=0, has_side_effects=True),
        )(positions, velocities, masses.reshape(1, -1), active.reshape(1, -1))

    spec = P(None, ("clusters", "blk"))
    flat = P(("clusters", "blk"))
    return jax.shard_map(
        shards,
        mesh=mesh,
        in_specs=(spec, spec, flat, flat),
        out_specs=(spec, spec, spec, spec),
        check_vma=False,
    )
```

```python
import functools

import jax
import jax.numpy as jnp
from jax import lax
from jax.experimental import pallas as pl
from jax.experimental.pallas import tpu as pltpu
from jax.sharding import PartitionSpec as P

STEPS = 2
TIME_STEP = 0.03125
ROWS = 32
F32 = jnp.float32
BF16 = jnp.bfloat16


def split3(value):
    high = value.astype(BF16)
    rest = value - high.astype(F32)
    middle = rest.astype(BF16)
    low = (rest - middle.astype(F32)).astype(BF16)
    return [high, middle, low]


def kernel(
    n,
    pos_ref,
    vel_ref,
    mass_ref,
    idx_ref,
    out_ref,
    slots,
    target,
    even,
    odd,
    right_even,
    right_odd,
    total,
    send_sem,
    recv_sem,
):
    me = lax.axis_index("blk")
    act = idx_ref.shape[1]
    stars = pos_ref.shape[1]

    half = n // 2
    core = me % 2

    def same_core(order):
        offset = ((order + 1) // 2) * (2 * (order % 2) - 1)
        return 2 * ((me // 2 + offset + half) % half) + core

    def greeted(j):
        first = (half - j) // half
        return first * (me + 1 - 2 * core) + (1 - first) * same_core(j)

    def peer_at(place):
        third = (place + half - 1) // half
        start = (n - place) // n
        second = (n - place) // (n - 1) - start
        k = place - third * (2 - third) + half * second
        other = k // half
        return same_core(k - other * half) + other * (1 - 2 * core)

    barrier = pltpu.get_barrier_semaphore()

    @pl.loop(0, half)
    def _(j):
        pl.semaphore_signal(
            barrier,
            inc=1,
            device_id={"blk": greeted(j)},
            device_id_type=pl.DeviceIdType.MESH,
        )

    local_idx = idx_ref[...] - me * stars
    table = jnp.concatenate(
        [pos_ref[...], vel_ref[...], mass_ref[...], jnp.zeros((1, stars), F32)], axis=0
    )
    pieces = jnp.concatenate(split3(table), axis=0)
    picked = (lax.broadcasted_iota(jnp.int32, (stars, act), 0) == local_idx).astype(F32).astype(BF16)
    found = jnp.dot(pieces, picked, preferred_element_type=F32)
    own = found[0:8] + found[8:16] + found[16:24]
    mass_rows = own[6:8]

    odd[...] = jnp.zeros_like(odd)
    pl.semaphore_wait(barrier, half)

    def copy_to(step, owner, target_id, j):
        return pltpu.make_async_remote_copy(
            src_ref=slots.at[step, owner],
            dst_ref=slots.at[step, owner],
            send_sem=send_sem.at[step, j],
            recv_sem=recv_sem.at[step, owner],
            device_id={"blk": target_id},
            device_id_type=pl.DeviceIdType.MESH,
        )

    def wait_at(step, place):
        peer = peer_at(place)
        copy_to(step, peer, greeted(0), 0).wait_recv()
        order = place - 1

        @pl.when((place > 1) & (place <= half))
        def _():
            copy_to(step, peer, greeted(0), half + order).start()

    row_id = lax.broadcasted_iota(jnp.int32, (8, act), 0)

    def weigh(source, weights, right, centre, fine):
        for side in range(act // 128):
            lanes = slice(side * 128, side * 128 + 128)
            src = [source[c : c + 1, lanes] for c in range(6)]
            for top in range(0, act, ROWS):
                rows = slice(top, top + ROWS)
                d = [src[c] - target[c, rows, :] for c in range(3)]
                e = [src[c + 3] - target[c + 3, rows, :] for c in range(3)]
                squared = d[0] * d[0] + d[1] * d[1] + d[2] * d[2] + 0.0025
                radial = d[0] * e[0] + d[1] * e[1] + d[2] * e[2]
                inverse = lax.rsqrt(squared)
                inverse2 = inverse * inverse
                w = inverse2 * inverse
                b = w * inverse2 * radial
                for value, down in ((w, 0), (b, act)):
                    high = value.astype(BF16)
                    out = slice(down + top, down + top + ROWS)
                    weights[out, lanes] = high
                    if fine:
                        low = (value - high.astype(F32)).astype(BF16)
                        weights[out, act + side * 128 : act + side * 128 + 128] = low
        factor = jnp.where(row_id == 6, 1.0, source - centre)
        splits = jnp.concatenate(split3(factor * source[6:7]), axis=0)
        right[:, 0:act] = splits
        if fine:
            right[:, act:] = splits

    def gather_sums(weights, right, fine):
        depth = 2 * act if fine else act
        total[...] += lax.dot_general(
            weights[:, 0:depth],
            right[:, 0:depth],
            (((1,), (1,)), ((), ())),
            preferred_element_type=F32,
        )

    def field(step, own):
        fine = step == STEPS
        slots[step, me] = own

        @pl.loop(0, half)
        def _(k):
            j = half - 1 - k
            copy_to(step, me, greeted(j), j).start()

        columns = own.T
        for c in range(6):
            target[c] = jnp.broadcast_to(columns[:, c : c + 1], (act, 128))
        centre = jnp.where(row_id[:, 0:1] < 6, jnp.mean(own, axis=1, keepdims=True), 0.0)
        total[...] = jnp.zeros_like(total)
        right_odd[...] = jnp.zeros_like(right_odd)

        @pl.loop(0, n // 2)
        def _(pair):
            first = 2 * pair

            @pl.when(pair > 0)
            def _():
                wait_at(step, first)

            wait_at(step, first + 1)
            gather_sums(odd, right_odd, fine)
            weigh(slots[step, peer_at(first)], even, right_even, centre, fine)
            gather_sums(even, right_even, fine)
            weigh(slots[step, peer_at(first + 1)], odd, right_odd, centre, fine)

        gather_sums(odd, right_odd, fine)
        sums = total[...].T
        sums = sums[0:8] + sums[8:16] + sums[16:24]
        plain, scaled = sums[:, 0:act], sums[:, act:]
        about = own - centre
        accel = plain[0:3] - about[0:3] * plain[6:7]
        jerk = (
            plain[3:6]
            - about[3:6] * plain[6:7]
            - 3.0 * (scaled[0:3] - about[0:3] * scaled[6:7])
        )
        return accel, jerk

    pos, vel = own[0:3], own[3:6]
    accel, jerk = field(0, own)
    h = TIME_STEP
    for step in range(STEPS):
        pred_pos = pos + h * vel + h**2 / 2.0 * accel + h**3 / 6.0 * jerk
        pred_vel = vel + h * accel + h**2 / 2.0 * jerk
        accel_new, jerk_new = field(
            step + 1, jnp.concatenate([pred_pos, pred_vel, mass_rows], axis=0)
        )
        vel_new = vel + h / 2.0 * (accel + accel_new) + h**2 / 12.0 * (jerk - jerk_new)
        pos = pos + h / 2.0 * (vel + vel_new) + h**2 / 12.0 * (accel - accel_new)
        vel, accel, jerk = vel_new, accel_new, jerk_new
    out_ref[...] = jnp.concatenate([pos, vel, accel, jerk], axis=0)

    for step in range(STEPS + 1):

        @pl.loop(0, half)
        def _(j):
            copy_to(step, me, greeted(j), j).wait_send()

        @pl.loop(1, half)
        def _(order):
            copy_to(step, same_core(order), greeted(0), half + order).wait_send()


def solution(mesh):
    n = mesh.shape["blk"]

    def shards(positions, velocities, masses, active):
        act = active.shape[0]
        vmem = pl.BlockSpec(memory_space=pltpu.VMEM)
        packed = pl.pallas_call(
            functools.partial(kernel, n),
            out_shape=jax.ShapeDtypeStruct((12, act), F32),
            in_specs=[vmem] * 4,
            out_specs=vmem,
            scratch_shapes=[
                pltpu.VMEM((STEPS + 1, n, 8, act), F32),
                pltpu.VMEM((6, act, 128), F32),
                pltpu.VMEM((2 * act, 2 * act), BF16),
                pltpu.VMEM((2 * act, 2 * act), BF16),
                pltpu.VMEM((24, 2 * act), BF16),
                pltpu.VMEM((24, 2 * act), BF16),
                pltpu.VMEM((2 * act, 24), F32),
                pltpu.SemaphoreType.DMA((STEPS + 1, n)),
                pltpu.SemaphoreType.DMA((STEPS + 1, n)),
            ],
            compiler_params=pltpu.CompilerParams(collective_id=0, has_side_effects=True),
        )(positions, velocities, masses.reshape(1, -1), active.reshape(1, -1))
        return packed[0:3], packed[3:6], packed[6:9], packed[9:12]

    spec = P(None, ("clusters", "blk"))
    flat = P(("clusters", "blk"))
    return jax.shard_map(
        shards,
        mesh=mesh,
        in_specs=(spec, spec, flat, flat),
        out_specs=(spec, spec, spec, spec),
        check_vma=False,
    )
```

```python
import functools

import jax
import jax.numpy as jnp
from jax import lax
from jax.experimental import pallas as pl
from jax.experimental.pallas import tpu as pltpu
from jax.sharding import PartitionSpec as P

STEPS = 2
TIME_STEP = 0.03125
ROWS = 32
F32 = jnp.float32
BF16 = jnp.bfloat16


def split3(value):
    high = value.astype(BF16)
    rest = value - high.astype(F32)
    middle = rest.astype(BF16)
    low = (rest - middle.astype(F32)).astype(BF16)
    return [high, middle, low]


def kernel(
    n,
    pos_ref,
    vel_ref,
    mass_ref,
    idx_ref,
    out_ref,
    slots,
    target,
    total,
    send_sem,
    recv_sem,
):
    me = lax.axis_index("blk")
    act = idx_ref.shape[1]
    stars = pos_ref.shape[1]

    half = n // 2
    core = me % 2

    chip = me // 2
    partner = me + 1 - 2 * core
    lead = min(4, (half - 1) // 2 * 2)

    def same_core(order, sign):
        offset = sign * ((order + 1) // 2) * (2 * (order % 2) - 1)
        return 2 * lax.rem(chip + (offset + half) % half, half) + core

    barrier = pltpu.get_barrier_semaphore()

    for peer in [partner] + [same_core(order, 1) for order in range(1, half)]:
        pl.semaphore_signal(
            barrier, inc=1, device_id={"blk": peer}, device_id_type=pl.DeviceIdType.MESH
        )

    local_idx = idx_ref[...] - me * stars
    table = jnp.concatenate(
        [pos_ref[...], vel_ref[...], mass_ref[...], jnp.zeros((1, stars), F32)], axis=0
    )
    pieces = jnp.concatenate(split3(table), axis=0)
    picked = (lax.broadcasted_iota(jnp.int32, (stars, act), 0) == local_idx).astype(F32).astype(BF16)
    found = jnp.dot(pieces, picked, preferred_element_type=F32)
    own = found[0:8] + found[8:16] + found[16:24]
    mass_rows = own[6:8]

    pl.semaphore_wait(barrier, half)

    def copy_to(step, source, place, peer):
        return pltpu.make_async_remote_copy(
            src_ref=slots.at[step, source],
            dst_ref=slots.at[step, place],
            send_sem=send_sem.at[step, place],
            recv_sem=recv_sem.at[step, place],
            device_id={"blk": peer},
            device_id_type=pl.DeviceIdType.MESH,
        )

    def wait_at(step, place):
        copy_to(step, place, place, partner).wait_recv()

        @pl.when((place > 1) & (place <= half))
        def _():
            copy_to(step, place, place + half - 1, partner).start()

    row_id = lax.broadcasted_iota(jnp.int32, (8, act), 0)

    def add_pair(blocks, centre, fine):
        right = []
        for block in blocks:
            factor = jnp.where(row_id == 6, 1.0, block - centre)
            right.append(jnp.concatenate(split3(factor * block[6:7]), axis=0))
        right = jnp.concatenate(right + right if fine else right, axis=1)
        for top in range(0, act, ROWS):
            rows = slice(top, top + ROWS)
            highs, lows = [], []
            for block in blocks:
                for side in range(0, act, 128):
                    src = [block[c : c + 1, side : side + 128] for c in range(6)]
                    d = [src[c] - target[c, rows, :] for c in range(3)]
                    e = [src[c + 3] - target[c + 3, rows, :] for c in range(3)]
                    squared = d[0] * d[0] + d[1] * d[1] + d[2] * d[2] + 0.0025
                    radial = d[0] * e[0] + d[1] * e[1] + d[2] * e[2]
                    inverse = lax.rsqrt(squared)
                    inverse2 = inverse * inverse
                    w = inverse2 * inverse
                    both = jnp.concatenate([w, w * inverse2 * radial], axis=0)
                    high = both.astype(BF16)
                    highs.append(high)
                    if fine:
                        lows.append((both - high.astype(F32)).astype(BF16))
            total[2 * top : 2 * top + 2 * ROWS] += lax.dot_general(
                jnp.concatenate(highs + lows, axis=1),
                right,
                (((1,), (1,)), ((), ())),
                preferred_element_type=F32,
            )

    def field(step, own):
        fine = step == STEPS
        slots[step, 0] = own
        for order in range(half - 1, 0, -1):
            copy_to(step, 0, 1 + order, same_core(order, -1)).start()
        copy_to(step, 0, 1, partner).start()

        columns = own.T
        for c in range(6):
            target[c] = jnp.broadcast_to(columns[:, c : c + 1], (act, 128))
        centre = jnp.where(row_id[:, 0:1] < 6, jnp.mean(own, axis=1, keepdims=True), 0.0)
        total[...] = jnp.zeros_like(total)

        @pl.loop(0, n // 2)
        def _(pair):
            middle = (pair > lead // 2) & (pair < (n - lead) // 2)
            first = jnp.where(middle, half + pair - lead // 2, 2 * pair)
            second = jnp.where(middle, 1 + lead + pair - lead // 2, 2 * pair + 1)

            @pl.when(pair > 0)
            def _():
                wait_at(step, first)

            wait_at(step, second)
            add_pair([slots[step, first], slots[step, second]], centre, fine)

        sums = total[...].T
        sums = sums[0:8] + sums[8:16] + sums[16:24]
        tops = range(0, 2 * act, 2 * ROWS)
        plain = jnp.concatenate([sums[:, t : t + ROWS] for t in tops], axis=1)
        scaled = jnp.concatenate([sums[:, t + ROWS : t + 2 * ROWS] for t in tops], axis=1)
        about = own - centre
        accel = plain[0:3] - about[0:3] * plain[6:7]
        jerk = (
            plain[3:6]
            - about[3:6] * plain[6:7]
            - 3.0 * (scaled[0:3] - about[0:3] * scaled[6:7])
        )
        return accel, jerk

    pos, vel = own[0:3], own[3:6]
    accel, jerk = field(0, own)
    h = TIME_STEP
    for step in range(STEPS):
        pred_pos = pos + h * vel + h**2 / 2.0 * accel + h**3 / 6.0 * jerk
        pred_vel = vel + h * accel + h**2 / 2.0 * jerk
        accel_new, jerk_new = field(
            step + 1, jnp.concatenate([pred_pos, pred_vel, mass_rows], axis=0)
        )
        vel_new = vel + h / 2.0 * (accel + accel_new) + h**2 / 12.0 * (jerk - jerk_new)
        pos = pos + h / 2.0 * (vel + vel_new) + h**2 / 12.0 * (accel - accel_new)
        vel, accel, jerk = vel_new, accel_new, jerk_new
    out_ref[...] = jnp.concatenate([pos, vel, accel, jerk], axis=0)

    for step in range(STEPS + 1):

        @pl.loop(1, n)
        def _(place):
            copy_to(step, 0, place, partner).wait_send()


def solution(mesh):
    n = mesh.shape["blk"]

    def shards(positions, velocities, masses, active):
        act = active.shape[0]
        vmem = pl.BlockSpec(memory_space=pltpu.VMEM)
        packed = pl.pallas_call(
            functools.partial(kernel, n),
            out_shape=jax.ShapeDtypeStruct((12, act), F32),
            in_specs=[vmem] * 4,
            out_specs=vmem,
            scratch_shapes=[
                pltpu.VMEM((STEPS + 1, n, 8, act), F32),
                pltpu.VMEM((6, act, 128), F32),
                pltpu.VMEM((2 * act, 24), F32),
                pltpu.SemaphoreType.DMA((STEPS + 1, n)),
                pltpu.SemaphoreType.DMA((STEPS + 1, n)),
            ],
            compiler_params=pltpu.CompilerParams(collective_id=0, has_side_effects=True),
        )(positions, velocities, masses.reshape(1, -1), active.reshape(1, -1))
        return packed[0:3], packed[3:6], packed[6:9], packed[9:12]

    spec = P(None, ("clusters", "blk"))
    flat = P(("clusters", "blk"))
    return jax.shard_map(
        shards,
        mesh=mesh,
        in_specs=(spec, spec, flat, flat),
        out_specs=(spec, spec, spec, spec),
        check_vma=False,
    )
```
